32 devices in a mesh: unit: 2 (over y), row: 4 (over x, core), col: 4 (over z).
Axes of the slice: x: 2, y: 2, z: 4, core: 2. Of those that a mesh axis runs over, the one named last changes fastest.
Arguments:
- tracer: float32 [4, 32, 64, 64], P('unit', None, 'row', 'col'), parts along dimension 0, may hold values from -6 to 6
- symbol_x: float32 [32], replicated, may hold values from 0.3 to 3
- symbol_y: float32 [64], replicated, may hold values from 0.3 to 3
- symbol_z: float32 [64], replicated, may hold values from 0.3 to 3
Outputs:
- smoothed: float32 [4, 32, 64, 64], P('unit', None, 'row', 'col'), parts along dimension 0
The draws below stay inside these ranges and needn't reach their ends.
There are 2 independent parts, one for each index of `unit`. The reference program is written for one: setup_inputs(seed, part) draws one part's arguments, and reference() takes and returns one part's arrays. A program takes and returns all parts, laid end to end along the dimension named above; an argument that names none is the same for every part. Nothing has to cross between parts.
All inputs are finite; a program needn't handle non-finite values.
Results may differ from the reference program's by a relative error of at most 0.0003.
Values sent between devices are 32-bit elements.
A program may use at most 64 MiB of HBM per device.

```python
import jax
import jax.numpy as jnp
from jax import lax

GRID_X = 32
GRID_Y = 64
GRID_Z = 64
FIELDS = 2


def levels(stream_key, extent, shards, smallest, top_value):
    def one(dim, shards_of):
        steps = jax.random.uniform(jax.random.fold_in(jax.random.fold_in(stream_key, 6), dim), (shards_of,), jnp.float32, smallest / len(shards), top_value / len(shards))
        return jnp.repeat(jnp.exp(steps), extent[dim] // shards_of).reshape((-1,) + (1,) * (len(extent) - dim - 1))

    factor_of = one(*shards[0])
    for cut in shards[1:]:
        factor_of = factor_of * one(*cut)
    return factor_of


def noise(key, extent, deviation, bound, split=(), dtype=jnp.bfloat16):
    level = levels(key, extent, split, -0.22, 0.18) if split else 1.0
    drawn = jax.random.normal(key, extent, jnp.float32) * deviation * level
    return jnp.minimum(jnp.maximum(drawn, -bound), bound).astype(dtype)


def setup_inputs(seed: int = 0, part: int = 0) -> dict:
    arg_keys = jax.random.split(jax.random.key(seed), 5)
    part_keys = jax.random.split(jax.random.fold_in(arg_keys[4], part), 5)
    return {
        "tracer": noise(part_keys[0], (FIELDS, GRID_X, GRID_Y, GRID_Z), 1.0, 6.0, ((2, 4), (3, 4)), jnp.float32),
        "symbol_x": jnp.clip(jax.random.uniform(arg_keys[1], (GRID_X,), jnp.float32, 0.3, 3.0), 0.3, 3.0),
        "symbol_y": jnp.clip(jax.random.uniform(arg_keys[2], (GRID_Y,), jnp.float32, 0.3, 3.0), 0.3, 3.0),
        "symbol_z": jnp.clip(jax.random.uniform(arg_keys[3], (GRID_Z,), jnp.float32, 0.3, 3.0), 0.3, 3.0),
    }


def mode_table(count):
    rank = jnp.arange(count)
    angle = jnp.pi / (4 * count) * ((2 * rank[:, None] + 1) * (2 * rank[None, :] + 1) % (8 * count)).astype(jnp.float32)
    return jnp.cos(angle) * (2.0 / count) ** 0.5

def to_modes(values, dim):
    moved = jnp.tensordot(values, mode_table(values.shape[dim]), axes=([dim], [0]), precision=lax.Precision.HIGHEST)
    return jnp.moveaxis(moved, -1, dim)

def reference(tracer, symbol_x, symbol_y, symbol_z):
    modes = tracer
    modes = to_modes(modes, 1)
    modes = to_modes(modes, 2)
    modes = to_modes(modes, 3)
    symbol = symbol_x[:, None, None] + symbol_y[None, :, None] + symbol_z[None, None, :]
    modes = modes * lax.rsqrt(symbol)
    smoothed = modes
    smoothed = to_modes(smoothed, 3)
    smoothed = to_modes(smoothed, 2)
    smoothed = to_modes(smoothed, 1)
    return smoothed
```

```python
import functools

import jax
import jax.numpy as jnp
import numpy as np
from jax import lax
from jax.experimental import pallas as pl
from jax.experimental.pallas import tpu as pltpu
from jax.sharding import PartitionSpec as P

MESH = pl.DeviceIdType.MESH
LANES = 128
ROWS = 8


def mode_table(count):
    rank = np.arange(count)
    angle = np.pi / (4 * count) * ((2 * rank[:, None] + 1) * (2 * rank[None, :] + 1) % (8 * count))
    return np.cos(angle) * (2.0 / count) ** 0.5


def two_parts(table):
    high = table.astype(jnp.bfloat16)
    low = (table - high.astype(np.float64)).astype(jnp.bfloat16)
    return np.stack([high, low])


def split(values):
    high = values.astype(jnp.bfloat16)
    return high, (values - high.astype(jnp.float32)).astype(jnp.bfloat16)


def dot(a, b):
    return jnp.dot(a, b, preferred_element_type=jnp.float32)


def right(values, table):
    rows = values.shape[0]
    high, low = split(values)
    both = dot(jnp.concatenate([high, low], axis=0), table[0])
    return both[:rows] + (both[rows:] + dot(high, table[1]))


def left(table, values):
    high, low = split(values)
    return dot(table, jnp.concatenate([high, high, low], axis=0))


def swap_blocks(tiles):
    count = len(tiles)
    block = LANES // count
    which = lax.broadcasted_iota(jnp.int32, tiles[0].shape, 1) // block
    out = []
    for j in range(count):
        tile = tiles[j]
        for i in range(count):
            if i != j:
                moved = pltpu.roll(tiles[i], ((i - j) * block) % LANES, 1)
                tile = jnp.where(which == i, moved, tile)
        out.append(tile)
    return out


def kernel(
    sizes, x_ref, sx_ref, sy_ref, sz_ref, wx_ref, wxt_ref, wy_ref, hz_ref, out_ref,
    send, recv, send_back, recv_back, send_sem, recv_sem, send_back_sem, recv_back_sem,
):
    fields, count_x, rows_n, cols_n, share_y, share_z, planes = sizes
    devices = rows_n * cols_n
    me = lax.axis_index("row") * cols_n + lax.axis_index("col")
    high_y, high_z = share_y // ROWS, share_z // ROWS
    groups = count_x // planes

    def place(index):
        return {"row": index // cols_n, "col": index % cols_n}

    barrier = pltpu.get_barrier_semaphore()
    for step in range(1, devices):
        peer = lax.rem(me + step, devices)
        pl.semaphore_signal(barrier, inc=1, device_id=place(peer), device_id_type=MESH)

    def exchange(source, target, source_sem, target_sem):
        copies = []
        for step in range(1, devices):
            peer = lax.rem(me + step, devices)
            copy = pltpu.make_async_remote_copy(
                src_ref=source.at[peer],
                dst_ref=target.at[me],
                send_sem=source_sem.at[peer],
                recv_sem=target_sem.at[me],
                device_id=place(peer),
                device_id_type=MESH,
            )
            copy.start()
            copies.append(copy)
        target[me] = source[me]
        return copies

    def arrive(copies, source, target, target_sem):
        for step in range(1, devices):
            peer = lax.rem(me + step, devices)
            pltpu.make_async_remote_copy(
                src_ref=source.at[peer],
                dst_ref=target.at[peer],
                send_sem=target_sem.at[peer],
                recv_sem=target_sem.at[peer],
                device_id=place(peer),
                device_id_type=MESH,
            ).wait_recv()

    packed = jnp.concatenate(
        [
            jnp.concatenate([x_ref[f * share_y + h * ROWS + y] for y in range(ROWS)], axis=1)
            for f in range(fields)
            for h in range(high_y)
        ],
        axis=0,
    )
    modes = right(packed, wx_ref)
    lane_tiles = count_x * ROWS // LANES
    per_tile = groups // lane_tiles

    def at(f, h, z, t):
        row = ((f * high_y + h) * high_z + z) * ROWS
        return modes[row : row + ROWS, t * LANES : (t + 1) * LANES]

    for f in range(fields):
        for t in range(lane_tiles):
            tiles = [at(f, h, z, t) for z in range(high_z) for h in range(high_y)]
            for i, tile in enumerate(swap_blocks(tiles)):
                send[f * groups + t * per_tile + i] = tile

    pl.semaphore_wait(barrier, devices - 1)
    copies = exchange(send, recv, send_sem, recv_sem)

    count_z, count_y = sz_ref.shape[1], sy_ref.shape[1]
    width = rows_n * high_y * planes * ROWS

    def column(row, size):
        diagonal = lax.broadcasted_iota(jnp.int32, (size, size), 0) == lax.broadcasted_iota(
            jnp.int32, (size, size), 1
        )
        return jnp.sum(jnp.where(diagonal, row, 0.0), axis=1, keepdims=True)

    symbol_z = column(sz_ref[...], count_z)
    lane = lax.broadcasted_iota(jnp.int32, (count_y, width), 1)
    rank = lane // (planes * ROWS) * ROWS + lane % ROWS
    chosen = rank == lax.broadcasted_iota(jnp.int32, (count_y, width), 0)
    symbol = jnp.sum(
        jnp.where(chosen, column(sy_ref[...], count_y), 0.0), axis=0, keepdims=True
    )
    plane = lax.broadcasted_iota(jnp.int32, (1, width), 1) // ROWS % planes
    first = lax.rem(me, groups) * planes
    symbol_x = jnp.zeros((1, width), jnp.float32)
    for p in range(planes):
        symbol_x = jnp.where(plane == p, sx_ref[first + p], symbol_x)
    factor = lax.rsqrt(symbol_x + symbol + symbol_z)

    arrive(copies, send, recv, recv_sem)

    lane_tiles = width // LANES
    grid = [[None] * lane_tiles for _ in range(cols_n * high_z)]
    for c in range(cols_n):
        for t in range(lane_tiles):
            tiles = [recv[(t * high_z + i) * cols_n + c] for i in range(high_z)]
            for z, tile in enumerate(swap_blocks(tiles)):
                grid[c * high_z + z][t] = tile
    block = jnp.concatenate([jnp.concatenate(row, axis=1) for row in grid], axis=0)
    block = right(block, wy_ref)
    block = left(hz_ref[...], block)
    block = block * factor
    block = left(hz_ref[...], block)
    block = right(block, wy_ref)
    for c in range(cols_n):
        for t in range(lane_tiles):
            tiles = [
                block[
                    (c * high_z + z) * ROWS : (c * high_z + z + 1) * ROWS,
                    t * LANES : (t + 1) * LANES,
                ]
                for z in range(high_z)
            ]
            for i, tile in enumerate(swap_blocks(tiles)):
                send_back[(t * high_z + i) * cols_n + c] = tile

    back_copies = exchange(send_back, recv_back, send_back_sem, recv_back_sem)
    for copy in copies:
        copy.wait_send()
    arrive(back_copies, send_back, recv_back, recv_back_sem)

    lane_tiles = count_x * ROWS // LANES
    grid = [[None] * lane_tiles for _ in range(fields * high_y * high_z)]
    for f in range(fields):
        for t in range(lane_tiles):
            tiles = [recv_back[f * groups + t * per_tile + i] for i in range(per_tile)]
            for i, tile in enumerate(swap_blocks(tiles)):
                z, h = divmod(i, high_y)
                grid[(f * high_y + h) * high_z + z][t] = tile
    modes = jnp.concatenate([jnp.concatenate(row, axis=1) for row in grid], axis=0)
    values = right(modes, wxt_ref)
    for f in range(fields):
        for h in range(high_y):
            row = (f * high_y + h) * share_z
            for y in range(ROWS):
                out_ref[f * share_y + h * ROWS + y] = values[
                    row : row + share_z, y * count_x : (y + 1) * count_x
                ]
    for copy in back_copies:
        copy.wait_send()


def fused(sizes, tracer, symbol_x, symbol_y, symbol_z):
    fields, count_x, rows_n, cols_n, share_y, share_z, planes = sizes
    devices = rows_n * cols_n
    count_y, count_z = symbol_y.shape[0], symbol_z.shape[0]
    high_y = share_y // ROWS

    table_x = np.einsum("xk,ab->axkb", mode_table(count_x), np.eye(ROWS))
    table_x = table_x.reshape(ROWS * count_x, count_x * ROWS)
    blocks = rows_n * high_y
    table_y = np.einsum(
        "aybz,kl->akyblz",
        mode_table(count_y).reshape(blocks, ROWS, blocks, ROWS),
        np.eye(planes),
    ).reshape(blocks * planes * ROWS, blocks * planes * ROWS)
    high, low = two_parts(mode_table(count_z))
    table_z = np.concatenate([high, low, high], axis=1)

    values = jnp.transpose(tracer, (0, 2, 3, 1)).reshape(fields * share_y, share_z, count_x)
    vmem = pl.BlockSpec(memory_space=pltpu.VMEM)
    smem = pl.BlockSpec(memory_space=pltpu.SMEM)
    tile = pltpu.VMEM((devices, ROWS, LANES), jnp.float32)
    out = pl.pallas_call(
        functools.partial(kernel, sizes),
        out_shape=jax.ShapeDtypeStruct(values.shape, jnp.float32),
        in_specs=[vmem, smem] + [vmem] * 6,
        out_specs=vmem,
        scratch_shapes=[tile] * 4 + [pltpu.SemaphoreType.DMA((devices,))] * 4,
        compiler_params=pltpu.CompilerParams(collective_id=0, has_side_effects=True),
    )(
        values,
        symbol_x,
        symbol_y.reshape(1, -1),
        symbol_z.reshape(1, -1),
        jnp.asarray(two_parts(table_x)),
        jnp.asarray(two_parts(table_x.T)),
        jnp.asarray(two_parts(table_y)),
        jnp.asarray(table_z),
    )
    out = out.reshape(fields, share_y, share_z, count_x)
    return jnp.transpose(out, (0, 3, 1, 2))


def to_modes(values, dim):
    table = jnp.asarray(mode_table(values.shape[dim]), jnp.float32)
    moved = jnp.tensordot(values, table, axes=([dim], [0]), precision=lax.Precision.HIGHEST)
    return jnp.moveaxis(moved, -1, dim)


def by_lines(values, symbol_x, symbol_y, symbol_z):
    values = to_modes(values, 1)
    values = lax.all_to_all(values, "row", split_axis=1, concat_axis=2, tiled=True)
    values = to_modes(values, 2)
    values = lax.all_to_all(values, "col", split_axis=2, concat_axis=3, tiled=True)
    values = to_modes(values, 3)
    share_x, share_y = values.shape[1], values.shape[2]
    part_x = lax.dynamic_slice_in_dim(symbol_x, lax.axis_index("row") * share_x, share_x)
    part_y = lax.dynamic_slice_in_dim(symbol_y, lax.axis_index("col") * share_y, share_y)
    symbol = part_x[:, None, None] + part_y[None, :, None] + symbol_z[None, None, :]
    values = values * lax.rsqrt(symbol)
    values = to_modes(values, 3)
    values = lax.all_to_all(values, "col", split_axis=3, concat_axis=2, tiled=True)
    values = to_modes(values, 2)
    values = lax.all_to_all(values, "row", split_axis=2, concat_axis=1, tiled=True)
    return to_modes(values, 1)


def solution(mesh):
    rows_n, cols_n = mesh.shape["row"], mesh.shape["col"]

    def shards(tracer, symbol_x, symbol_y, symbol_z):
        fields, count_x, share_y, share_z = tracer.shape
        planes = fields * count_x // (rows_n * cols_n)
        high_y, high_z = share_y // ROWS, share_z // ROWS
        whole_tiles = (
            planes * rows_n * cols_n == fields * count_x
            and count_x % planes == 0
            and high_y * ROWS == share_y
            and high_z * ROWS == share_z
            and planes * ROWS * high_y * high_z == LANES
            and count_x * ROWS % LANES == 0
            and rows_n % high_z == 0
        )
        if not whole_tiles:
            return by_lines(tracer, symbol_x, symbol_y, symbol_z)
        sizes = fields, count_x, rows_n, cols_n, share_y, share_z, planes
        return fused(sizes, tracer, symbol_x, symbol_y, symbol_z)

    in_specs = (P("unit", None, "row", "col"), P(), P(), P())
    out_specs = P("unit", None, "row", "col")
    return jax.shard_map(shards, mesh=mesh, in_specs=in_specs, out_specs=out_specs, check_vma=False)
```

```python
import functools

import jax
import jax.numpy as jnp
import numpy as np
from jax import lax
from jax.experimental import pallas as pl
from jax.experimental.pallas import tpu as pltpu
from jax.sharding import PartitionSpec as P

MESH = pl.DeviceIdType.MESH
LANES = 128
ROWS = 8
VMEM_BYTES = 16 * 2**20


def mode_table(count):
    rank = np.arange(count)
    angle = np.pi / (4 * count) * ((2 * rank[:, None] + 1) * (2 * rank[None, :] + 1) % (8 * count))
    return np.cos(angle) * (2.0 / count) ** 0.5


def two_parts(table):
    high = table.astype(jnp.bfloat16)
    low = (table - high.astype(np.float64)).astype(jnp.bfloat16)
    return np.stack([high, low])


def split(values):
    high = values.astype(jnp.bfloat16)
    return high, (values - high.astype(jnp.float32)).astype(jnp.bfloat16)


def dot(a, b):
    return jnp.dot(a, b, preferred_element_type=jnp.float32)


def right(values, table):
    rows = values.shape[0]
    high, low = split(values)
    both = dot(jnp.concatenate([high, low], axis=0), table[0])
    return both[:rows] + (both[rows:] + dot(high, table[1]))


def left(table, values):
    high, low = split(values)
    return dot(table, jnp.concatenate([high, high, low], axis=0))


def swap_blocks(tiles):
    count = len(tiles)
    block = LANES // count
    which = lax.broadcasted_iota(jnp.int32, tiles[0].shape, 1) // block
    out = []
    for j in range(count):
        tile = tiles[j]
        for i in range(count):
            if i != j:
                moved = pltpu.roll(tiles[i], ((i - j) * block) % LANES, 1)
                tile = jnp.where(which == i, moved, tile)
        out.append(tile)
    return out


def kernel(
    sizes, x_hbm, sx_ref, sy_hbm, sz_hbm, wx_hbm, wy_hbm, hz_hbm, recv_back,
    x_ref, sy_ref, sz_ref, wx_ref, wy_ref, hz_ref, send, recv, send_back,
    load_sem, send_sem, recv_sem, send_back_sem, recv_back_sem,
):
    fields, count_x, rows_n, cols_n, share_y, share_z, planes = sizes
    devices = rows_n * cols_n
    me = lax.axis_index("row") * cols_n + lax.axis_index("col")
    high_y, high_z = share_y // ROWS, share_z // ROWS
    groups = count_x // planes

    def place(index):
        return {"row": index // cols_n, "col": index % cols_n}

    barrier = pltpu.get_barrier_semaphore()
    for step in range(1, devices):
        peer = lax.rem(me + step, devices)
        pl.semaphore_signal(barrier, inc=1, device_id=place(peer), device_id_type=MESH)

    loads = [
        pltpu.make_async_copy(source, target, load_sem.at[i])
        for i, (source, target) in enumerate(
            [
                (x_hbm, x_ref),
                (wx_hbm, wx_ref),
                (sy_hbm, sy_ref),
                (sz_hbm, sz_ref),
                (wy_hbm, wy_ref),
                (hz_hbm, hz_ref),
            ]
        )
    ]
    for load in loads:
        load.start()

    def exchange(source, target, source_sem, target_sem):
        copies = []
        for step in range(1, devices):
            peer = lax.rem(me + step, devices)
            copy = pltpu.make_async_remote_copy(
                src_ref=source.at[peer],
                dst_ref=target.at[me],
                send_sem=source_sem.at[peer],
                recv_sem=target_sem.at[me],
                device_id=place(peer),
                device_id_type=MESH,
            )
            copy.start()
            copies.append(copy)
        target[me] = source[me]
        return copies

    def arrive(copies, source, target, target_sem):
        for step in range(1, devices):
            peer = lax.rem(me + step, devices)
            pltpu.make_async_remote_copy(
                src_ref=source.at[peer],
                dst_ref=target.at[peer],
                send_sem=target_sem.at[peer],
                recv_sem=target_sem.at[peer],
                device_id=place(peer),
                device_id_type=MESH,
            ).wait_recv()

    loads[0].wait()
    loads[1].wait()
    packed = jnp.concatenate(
        [
            jnp.concatenate([x_ref[f * share_y + h * ROWS + y] for y in range(ROWS)], axis=1)
            for f in range(fields)
            for h in range(high_y)
        ],
        axis=0,
    )
    modes = right(packed, wx_ref)
    lane_tiles = count_x * ROWS // LANES
    per_tile = groups // lane_tiles

    def at(f, h, z, t):
        row = ((f * high_y + h) * high_z + z) * ROWS
        return modes[row : row + ROWS, t * LANES : (t + 1) * LANES]

    for f in range(fields):
        for t in range(lane_tiles):
            tiles = [at(f, h, z, t) for z in range(high_z) for h in range(high_y)]
            for i, tile in enumerate(swap_blocks(tiles)):
                send[f * groups + t * per_tile + i] = tile

    pl.semaphore_wait(barrier, devices - 1)
    copies = exchange(send, recv, send_sem, recv_sem)

    for load in loads[2:]:
        load.wait()
    count_z, count_y = sz_ref.shape[1], sy_ref.shape[1]
    width = rows_n * high_y * planes * ROWS

    def column(row, size):
        diagonal = lax.broadcasted_iota(jnp.int32, (size, size), 0) == lax.broadcasted_iota(
            jnp.int32, (size, size), 1
        )
        return jnp.sum(jnp.where(diagonal, row, 0.0), axis=1, keepdims=True)

    symbol_z = column(sz_ref[...], count_z)
    lane = lax.broadcasted_iota(jnp.int32, (count_y, width), 1)
    rank = lane // (planes * ROWS) * ROWS + lane % ROWS
    chosen = rank == lax.broadcasted_iota(jnp.int32, (count_y, width), 0)
    symbol = jnp.sum(
        jnp.where(chosen, column(sy_ref[...], count_y), 0.0), axis=0, keepdims=True
    )
    plane = lax.broadcasted_iota(jnp.int32, (1, width), 1) // ROWS % planes
    first = lax.rem(me, groups) * planes
    symbol_x = jnp.zeros((1, width), jnp.float32)
    for p in range(planes):
        symbol_x = jnp.where(plane == p, sx_ref[first + p], symbol_x)
    factor = lax.rsqrt(symbol_x + symbol + symbol_z)

    arrive(copies, send, recv, recv_sem)

    lane_tiles = width // LANES
    grid = [[None] * lane_tiles for _ in range(cols_n * high_z)]
    for c in range(cols_n):
        for t in range(lane_tiles):
            tiles = [recv[(t * high_z + i) * cols_n + c] for i in range(high_z)]
            for z, tile in enumerate(swap_blocks(tiles)):
                grid[c * high_z + z][t] = tile
    block = jnp.concatenate([jnp.concatenate(row, axis=1) for row in grid], axis=0)
    block = right(block, wy_ref)
    block = left(hz_ref[...], block)
    block = block * factor
    block = left(hz_ref[...], block)
    block = right(block, wy_ref)
    for c in range(cols_n):
        for t in range(lane_tiles):
            tiles = [
                block[
                    (c * high_z + z) * ROWS : (c * high_z + z + 1) * ROWS,
                    t * LANES : (t + 1) * LANES,
                ]
                for z in range(high_z)
            ]
            for i, tile in enumerate(swap_blocks(tiles)):
                send_back[(t * high_z + i) * cols_n + c] = tile

    back_copies = exchange(send_back, recv_back, send_back_sem, recv_back_sem)
    for copy in copies:
        copy.wait_send()
    arrive(back_copies, send_back, recv_back, recv_back_sem)
    for copy in back_copies:
        copy.wait_send()


def finish(sizes, tiles_ref, wxt_ref, out_ref):
    fields, count_x, rows_n, cols_n, share_y, share_z, planes = sizes
    high_y, high_z = share_y // ROWS, share_z // ROWS
    groups = count_x // planes
    lane_tiles = count_x * ROWS // LANES
    per_tile = groups // lane_tiles
    grid = [[None] * lane_tiles for _ in range(fields * high_y * high_z)]
    for f in range(fields):
        for t in range(lane_tiles):
            tiles = [tiles_ref[f * groups + t * per_tile + i] for i in range(per_tile)]
            for i, tile in enumerate(swap_blocks(tiles)):
                z, h = divmod(i, high_y)
                grid[(f * high_y + h) * high_z + z][t] = tile
    modes = jnp.concatenate([jnp.concatenate(row, axis=1) for row in grid], axis=0)
    values = right(modes, wxt_ref)
    for f in range(fields):
        for h in range(high_y):
            row = (f * high_y + h) * share_z
            for y in range(ROWS):
                out_ref[f * share_y + h * ROWS + y] = values[
                    row : row + share_z, y * count_x : (y + 1) * count_x
                ]


def fused(sizes, tracer, symbol_x, symbol_y, symbol_z):
    fields, count_x, rows_n, cols_n, share_y, share_z, planes = sizes
    devices = rows_n * cols_n
    count_y, count_z = symbol_y.shape[0], symbol_z.shape[0]
    high_y = share_y // ROWS

    table_x = np.einsum("xk,ab->axkb", mode_table(count_x), np.eye(ROWS))
    table_x = table_x.reshape(ROWS * count_x, count_x * ROWS)
    blocks = rows_n * high_y
    table_y = np.einsum(
        "aybz,kl->akyblz",
        mode_table(count_y).reshape(blocks, ROWS, blocks, ROWS),
        np.eye(planes),
    ).reshape(blocks * planes * ROWS, blocks * planes * ROWS)
    high, low = two_parts(mode_table(count_z))
    table_z = np.concatenate([high, low, high], axis=1)

    values = jnp.transpose(tracer, (0, 2, 3, 1)).reshape(fields * share_y, share_z, count_x)
    hbm = pl.BlockSpec(memory_space=pltpu.HBM)
    vmem = pl.BlockSpec(memory_space=pltpu.VMEM)
    smem = pl.BlockSpec(memory_space=pltpu.SMEM)
    tiles = jax.ShapeDtypeStruct((devices, ROWS, LANES), jnp.float32)
    operands = (
        values,
        symbol_x,
        symbol_y.reshape(1, -1),
        symbol_z.reshape(1, -1),
        jnp.asarray(two_parts(table_x)),
        jnp.asarray(two_parts(table_y)),
        jnp.asarray(table_z),
    )
    held = [pltpu.VMEM(o.shape, o.dtype) for i, o in enumerate(operands) if i != 1]
    back = pl.pallas_call(
        functools.partial(kernel, sizes),
        out_shape=tiles,
        in_specs=[hbm, smem] + [hbm] * 5,
        out_specs=vmem,
        scratch_shapes=held
        + [pltpu.VMEM(tiles.shape, tiles.dtype)] * 3
        + [pltpu.SemaphoreType.DMA((len(held),))]
        + [pltpu.SemaphoreType.DMA((devices,))] * 4,
        compiler_params=pltpu.CompilerParams(
            collective_id=0, has_side_effects=True, vmem_limit_bytes=VMEM_BYTES
        ),
    )(*operands)
    out = pl.pallas_call(
        functools.partial(finish, sizes),
        out_shape=jax.ShapeDtypeStruct(values.shape, jnp.float32),
        in_specs=[vmem, vmem],
        out_specs=vmem,
        compiler_params=pltpu.CompilerParams(vmem_limit_bytes=VMEM_BYTES),
    )(back, jnp.asarray(two_parts(table_x.T)))
    out = out.reshape(fields, share_y, share_z, count_x)
    return jnp.transpose(out, (0, 3, 1, 2))


def to_modes(values, dim):
    table = jnp.asarray(mode_table(values.shape[dim]), jnp.float32)
    moved = jnp.tensordot(values, table, axes=([dim], [0]), precision=lax.Precision.HIGHEST)
    return jnp.moveaxis(moved, -1, dim)


def by_lines(values, symbol_x, symbol_y, symbol_z):
    values = to_modes(values, 1)
    values = lax.all_to_all(values, "row", split_axis=1, concat_axis=2, tiled=True)
    values = to_modes(values, 2)
    values = lax.all_to_all(values, "col", split_axis=2, concat_axis=3, tiled=True)
    values = to_modes(values, 3)
    share_x, share_y = values.shape[1], values.shape[2]
    part_x = lax.dynamic_slice_in_dim(symbol_x, lax.axis_index("row") * share_x, share_x)
    part_y = lax.dynamic_slice_in_dim(symbol_y, lax.axis_index("col") * share_y, share_y)
    symbol = part_x[:, None, None] + part_y[None, :, None] + symbol_z[None, None, :]
    values = values * lax.rsqrt(symbol)
    values = to_modes(values, 3)
    values = lax.all_to_all(values, "col", split_axis=3, concat_axis=2, tiled=True)
    values = to_modes(values, 2)
    values = lax.all_to_all(values, "row", split_axis=2, concat_axis=1, tiled=True)
    return to_modes(values, 1)


def solution(mesh):
    rows_n, cols_n = mesh.shape["row"], mesh.shape["col"]

    def shards(tracer, symbol_x, symbol_y, symbol_z):
        fields, count_x, share_y, share_z = tracer.shape
        planes = fields * count_x // (rows_n * cols_n)
        high_y, high_z = share_y // ROWS, share_z // ROWS
        whole_tiles = (
            planes * rows_n * cols_n == fields * count_x
            and count_x % planes == 0
            and high_y * ROWS == share_y
            and high_z * ROWS == share_z
            and planes * ROWS * high_y * high_z == LANES
            and count_x * ROWS % LANES == 0
            and rows_n % high_z == 0
        )
        if not whole_tiles:
            return by_lines(tracer, symbol_x, symbol_y, symbol_z)
        sizes = fields, count_x, rows_n, cols_n, share_y, share_z, planes
        return fused(sizes, tracer, symbol_x, symbol_y, symbol_z)

    in_specs = (P("unit", None, "row", "col"), P(), P(), P())
    out_specs = P("unit", None, "row", "col")
    return jax.shard_map(shards, mesh=mesh, in_specs=in_specs, out_specs=out_specs, check_vma=False)
```

```python
import functools

import jax
import jax.numpy as jnp
import numpy as np
from jax import lax
from jax.experimental import pallas as pl
from jax.experimental.pallas import tpu as pltpu
from jax.sharding import PartitionSpec as P

MESH = pl.DeviceIdType.MESH
LANES = 128
ROWS = 8


def mode_table(count):
    rank = np.arange(count)
    angle = np.pi / (4 * count) * ((2 * rank[:, None] + 1) * (2 * rank[None, :] + 1) % (8 * count))
    return np.cos(angle) * (2.0 / count) ** 0.5


def two_parts(table):
    high = table.astype(jnp.bfloat16)
    low = (table - high.astype(np.float64)).astype(jnp.bfloat16)
    return np.stack([high, low])


def split(values):
    high = values.astype(jnp.bfloat16)
    return high, (values - high.astype(jnp.float32)).astype(jnp.bfloat16)


def dot(a, b):
    return jnp.dot(a, b, preferred_element_type=jnp.float32)


def right(values, table):
    rows = values.shape[0]
    high, low = split(values)
    both = dot(jnp.concatenate([high, low], axis=0), table[0])
    return both[:rows] + (both[rows:] + dot(high, table[1]))


def left(table, values):
    high, low = split(values)
    return dot(table, jnp.concatenate([high, high, low], axis=0))


def swap_blocks(tiles):
    count = len(tiles)
    block = LANES // count
    which = lax.broadcasted_iota(jnp.int32, tiles[0].shape, 1) // block
    out = []
    for j in range(count):
        tile = tiles[j]
        for i in range(count):
            if i != j:
                moved = pltpu.roll(tiles[i], ((i - j) * block) % LANES, 1)
                tile = jnp.where(which == i, moved, tile)
        out.append(tile)
    return out


def kernel(
    sizes, x_hbm, sx_ref, sy_hbm, sz_hbm, wx_hbm, wy_hbm, hz_hbm, recv_back,
    x_ref, sy_ref, sz_ref, wx_ref, wy_ref, hz_ref, send, recv, send_back,
    load_sem, send_sem, recv_sem, send_back_sem, recv_back_sem,
):
    fields, count_x, rows_n, cols_n, share_y, share_z, planes = sizes
    devices = rows_n * cols_n
    me = lax.axis_index("row") * cols_n + lax.axis_index("col")
    high_y, high_z = share_y // ROWS, share_z // ROWS
    groups = count_x // planes

    def place(index):
        return {"row": index // cols_n, "col": index % cols_n}

    barrier = pltpu.get_barrier_semaphore()
    for step in range(1, devices):
        peer = lax.rem(me + step, devices)
        pl.semaphore_signal(barrier, inc=1, device_id=place(peer), device_id_type=MESH)

    loads = [
        pltpu.make_async_copy(source, target, load_sem.at[i])
        for i, (source, target) in enumerate(
            [
                (x_hbm, x_ref),
                (wx_hbm, wx_ref),
                (sy_hbm, sy_ref),
                (sz_hbm, sz_ref),
                (wy_hbm, wy_ref),
                (hz_hbm, hz_ref),
            ]
        )
    ]
    for load in loads:
        load.start()

    def exchange(source, target, source_sem, target_sem):
        copies = []
        for step in range(1, devices):
            peer = lax.rem(me + step, devices)
            copy = pltpu.make_async_remote_copy(
                src_ref=source.at[peer],
                dst_ref=target.at[me],
                send_sem=source_sem.at[peer],
                recv_sem=target_sem.at[me],
                device_id=place(peer),
                device_id_type=MESH,
            )
            copy.start()
            copies.append(copy)
        target[me] = source[me]
        return copies

    def arrive(copies, source, target, target_sem):
        for step in range(1, devices):
            peer = lax.rem(me + step, devices)
            pltpu.make_async_remote_copy(
                src_ref=source.at[peer],
                dst_ref=target.at[peer],
                send_sem=target_sem.at[peer],
                recv_sem=target_sem.at[peer],
                device_id=place(peer),
                device_id_type=MESH,
            ).wait_recv()

    loads[0].wait()
    loads[1].wait()
    packed = jnp.concatenate(
        [
            jnp.concatenate([x_ref[f * share_y + h * ROWS + y] for y in range(ROWS)], axis=1)
            for f in range(fields)
            for h in range(high_y)
        ],
        axis=0,
    )
    modes = right(packed, wx_ref)
    lane_tiles = count_x * ROWS // LANES
    per_tile = groups // lane_tiles

    def at(f, h, z, t):
        row = ((f * high_y + h) * high_z + z) * ROWS
        return modes[row : row + ROWS, t * LANES : (t + 1) * LANES]

    for f in range(fields):
        for t in range(lane_tiles):
            tiles = [at(f, h, z, t) for z in range(high_z) for h in range(high_y)]
            for i, tile in enumerate(swap_blocks(tiles)):
                send[f * groups + t * per_tile + i] = tile

    pl.semaphore_wait(barrier, devices - 1)
    copies = exchange(send, recv, send_sem, recv_sem)

    for load in loads[2:]:
        load.wait()
    count_z, count_y = sz_ref.shape[1], sy_ref.shape[1]
    width = rows_n * high_y * planes * ROWS

    def column(row, size):
        diagonal = lax.broadcasted_iota(jnp.int32, (size, size), 0) == lax.broadcasted_iota(
            jnp.int32, (size, size), 1
        )
        return jnp.sum(jnp.where(diagonal, row, 0.0), axis=1, keepdims=True)

    symbol_z = column(sz_ref[...], count_z)
    lane = lax.broadcasted_iota(jnp.int32, (count_y, width), 1)
    rank = lane // (planes * ROWS) * ROWS + lane % ROWS
    chosen = rank == lax.broadcasted_iota(jnp.int32, (count_y, width), 0)
    symbol = jnp.sum(
        jnp.where(chosen, column(sy_ref[...], count_y), 0.0), axis=0, keepdims=True
    )
    plane = lax.broadcasted_iota(jnp.int32, (1, width), 1) // ROWS % planes
    first = lax.rem(me, groups) * planes
    symbol_x = jnp.zeros((1, width), jnp.float32)
    for p in range(planes):
        symbol_x = jnp.where(plane == p, sx_ref[first + p], symbol_x)
    factor = lax.rsqrt(symbol_x + symbol + symbol_z)

    arrive(copies, send, recv, recv_sem)

    lane_tiles = width // LANES
    grid = [[None] * lane_tiles for _ in range(cols_n * high_z)]
    for c in range(cols_n):
        for t in range(lane_tiles):
            tiles = [recv[(t * high_z + i) * cols_n + c] for i in range(high_z)]
            for z, tile in enumerate(swap_blocks(tiles)):
                grid[c * high_z + z][t] = tile
    block = jnp.concatenate([jnp.concatenate(row, axis=1) for row in grid], axis=0)
    block = right(block, wy_ref)
    block = left(hz_ref[...], block)
    block = block * factor
    block = left(hz_ref[...], block)
    block = right(block, wy_ref)
    for c in range(cols_n):
        for t in range(lane_tiles):
            tiles = [
                block[
                    (c * high_z + z) * ROWS : (c * high_z + z + 1) * ROWS,
                    t * LANES : (t + 1) * LANES,
                ]
                for z in range(high_z)
            ]
            for i, tile in enumerate(swap_blocks(tiles)):
                send_back[(t * high_z + i) * cols_n + c] = tile

    back_copies = exchange(send_back, recv_back, send_back_sem, recv_back_sem)
    for copy in copies:
        copy.wait_send()
    arrive(back_copies, send_back, recv_back, recv_back_sem)
    for copy in back_copies:
        copy.wait_send()


def finish(sizes, tiles_ref, wxt_ref, out_ref):
    fields, count_x, rows_n, cols_n, share_y, share_z, planes = sizes
    high_y, high_z = share_y // ROWS, share_z // ROWS
    groups = count_x // planes
    lane_tiles = count_x * ROWS // LANES
    per_tile = groups // lane_tiles
    grid = [[None] * lane_tiles for _ in range(fields * high_y * high_z)]
    for f in range(fields):
        for t in range(lane_tiles):
            tiles = [tiles_ref[f * groups + t * per_tile + i] for i in range(per_tile)]
            for i, tile in enumerate(swap_blocks(tiles)):
                z, h = divmod(i, high_y)
                grid[(f * high_y + h) * high_z + z][t] = tile
    modes = jnp.concatenate([jnp.concatenate(row, axis=1) for row in grid], axis=0)
    values = right(modes, wxt_ref)
    for f in range(fields):
        for h in range(high_y):
            row = (f * high_y + h) * share_z
            for y in range(ROWS):
                out_ref[f * share_y + h * ROWS + y] = values[
                    row : row + share_z, y * count_x : (y + 1) * count_x
                ]


def fused(sizes, tracer, symbol_x, symbol_y, symbol_z):
    fields, count_x, rows_n, cols_n, share_y, share_z, planes = sizes
    devices = rows_n * cols_n
    count_y, count_z = symbol_y.shape[0], symbol_z.shape[0]
    high_y = share_y // ROWS

    table_x = np.einsum("xk,ab->axkb", mode_table(count_x), np.eye(ROWS))
    table_x = table_x.reshape(ROWS * count_x, count_x * ROWS)
    blocks = rows_n * high_y
    table_y = np.einsum(
        "aybz,kl->akyblz",
        mode_table(count_y).reshape(blocks, ROWS, blocks, ROWS),
        np.eye(planes),
    ).reshape(blocks * planes * ROWS, blocks * planes * ROWS)
    high, low = two_parts(mode_table(count_z))
    table_z = np.concatenate([high, low, high], axis=1)

    values = jnp.transpose(tracer, (0, 2, 3, 1)).reshape(fields * share_y, share_z, count_x)
    hbm = pl.BlockSpec(memory_space=pltpu.HBM)
    vmem = pl.BlockSpec(memory_space=pltpu.VMEM)
    smem = pl.BlockSpec(memory_space=pltpu.SMEM)
    tiles = jax.ShapeDtypeStruct((devices, ROWS, LANES), jnp.float32)
    operands = (
        values,
        symbol_x,
        symbol_y.reshape(1, -1),
        symbol_z.reshape(1, -1),
        jnp.asarray(two_parts(table_x)),
        jnp.asarray(two_parts(table_y)),
        jnp.asarray(table_z),
    )
    held = [pltpu.VMEM(o.shape, o.dtype) for i, o in enumerate(operands) if i != 1]
    back = pl.pallas_call(
        functools.partial(kernel, sizes),
        out_shape=tiles,
        in_specs=[hbm, smem] + [hbm] * 5,
        out_specs=vmem,
        scratch_shapes=held
        + [pltpu.VMEM(tiles.shape, tiles.dtype)] * 3
        + [pltpu.SemaphoreType.DMA((len(held),))]
        + [pltpu.SemaphoreType.DMA((devices,))] * 4,
        compiler_params=pltpu.CompilerParams(
            collective_id=0, has_side_effects=True
        ),
    )(*operands)
    out = pl.pallas_call(
        functools.partial(finish, sizes),
        out_shape=jax.ShapeDtypeStruct(values.shape, jnp.float32),
        in_specs=[vmem, vmem],
        out_specs=vmem,
        compiler_params=pltpu.CompilerParams(),
    )(back, jnp.asarray(two_parts(table_x.T)))
    out = out.reshape(fields, share_y, share_z, count_x)
    return jnp.transpose(out, (0, 3, 1, 2))


def to_modes(values, dim):
    table = jnp.asarray(mode_table(values.shape[dim]), jnp.float32)
    moved = jnp.tensordot(values, table, axes=([dim], [0]), precision=lax.Precision.HIGHEST)
    return jnp.moveaxis(moved, -1, dim)


def by_lines(values, symbol_x, symbol_y, symbol_z):
    values = to_modes(values, 1)
    values = lax.all_to_all(values, "row", split_axis=1, concat_axis=2, tiled=True)
    values = to_modes(values, 2)
    values = lax.all_to_all(values, "col", split_axis=2, concat_axis=3, tiled=True)
    values = to_modes(values, 3)
    share_x, share_y = values.shape[1], values.shape[2]
    part_x = lax.dynamic_slice_in_dim(symbol_x, lax.axis_index("row") * share_x, share_x)
    part_y = lax.dynamic_slice_in_dim(symbol_y, lax.axis_index("col") * share_y, share_y)
    symbol = part_x[:, None, None] + part_y[None, :, None] + symbol_z[None, None, :]
    values = values * lax.rsqrt(symbol)
    values = to_modes(values, 3)
    values = lax.all_to_all(values, "col", split_axis=3, concat_axis=2, tiled=True)
    values = to_modes(values, 2)
    values = lax.all_to_all(values, "row", split_axis=2, concat_axis=1, tiled=True)
    return to_modes(values, 1)


def solution(mesh):
    rows_n, cols_n = mesh.shape["row"], mesh.shape["col"]

    def shards(tracer, symbol_x, symbol_y, symbol_z):
        fields, count_x, share_y, share_z = tracer.shape
        planes = fields * count_x // (rows_n * cols_n)
        high_y, high_z = share_y // ROWS, share_z // ROWS
        whole_tiles = (
            planes * rows_n * cols_n == fields * count_x
            and count_x % planes == 0
            and high_y * ROWS == share_y
            and high_z * ROWS == share_z
            and planes * ROWS * high_y * high_z == LANES
            and count_x * ROWS % LANES == 0
            and rows_n % high_z == 0
        )
        if not whole_tiles:
            return by_lines(tracer, symbol_x, symbol_y, symbol_z)
        sizes = fields, count_x, rows_n, cols_n, share_y, share_z, planes
        return fused(sizes, tracer, symbol_x, symbol_y, symbol_z)

    in_specs = (P("unit", None, "row", "col"), P(), P(), P())
    out_specs = P("unit", None, "row", "col")
    return jax.shard_map(shards, mesh=mesh, in_specs=in_specs, out_specs=out_specs, check_vma=False)
```
